32 devices in a mesh: freq: 16 (over z, y, x), depth: 2 (over core).
Axes of the slice: x: 2, y: 2, z: 4, core: 2. Of those that a mesh axis runs over, the one named last changes fastest.
Arguments:
- pressure_field: bfloat16 [8192, 4096], P('depth', 'freq'), may hold values from -6 to 6
- block_main: bfloat16 [8192, 3, 2, 128], P('depth'), may hold values from -0.15625 to 0.15625
- block_coupled: bfloat16 [8192, 3, 2, 128], P('depth'), may hold values from -0.15625 to 0.15625
- coupling: float32 [4096], P('freq'), may hold values from -3 to 3
- frequencies: float32 [2048], replicated, may hold values from 1 to 1024
- receivers: int32 [512], replicated, may hold values from 0 to 8191
- floors: int32 [4], replicated, may hold values from 2048 to 8191
Outputs:
- series: float32 [512, 2048], P('depth', 'freq')
The draws below stay inside these ranges and needn't reach their ends.
Inputs may be any that keep to these rules, and one draw needn't show every extreme that they name: `receivers`: any depth cells, repeats possible.
All inputs are finite; a program needn't handle non-finite values.
Results may differ from the reference program's by a relative error of at most 0.0061.
Values may be sent and summed in bfloat16 or wider, within the bound.
A program may use at most 256 MiB of HBM per device.

```python
import math
import jax
import jax.numpy as jnp
from jax import lax

NZ = 8192
BS = 128
NT = 2048
R = 512
STEPS = 4
F_DEV = 128
F = 2048
N_FREQ = 16


def touch_ends(array, key, smallest, largest):
    index_at = [jax.random.randint(jax.random.fold_in(key, axis), (), 0, length) for axis, length in enumerate(array.shape)]
    main_axis = array.shape.index(max(array.shape))
    next_to = index_at[:main_axis] + [(index_at[main_axis] + 1) % array.shape[main_axis]] + index_at[main_axis + 1:]
    return array.at[tuple(index_at)].set(smallest).at[tuple(next_to)].set(largest)


def levels(own_key, shape, cuts, least, top_value):
    level = 1.0
    for position, blocks in cuts:
        draws = jax.random.uniform(jax.random.fold_in(jax.random.fold_in(own_key, 6), position), (blocks,), jnp.float32, least / len(cuts), top_value / len(cuts))
        level = level * jnp.repeat(jnp.exp(draws), shape[position] // blocks).reshape((-1,) + (1,) * (len(shape) - 1 - position))
    return level


def gaussian(stream_key, dims, scale, reach, split=(), held_as=jnp.bfloat16):
    entries = scale * jax.random.normal(stream_key, dims, jnp.float32)
    if split:
        entries = entries * levels(stream_key, dims, split, -0.22, 0.18)
    return jnp.clip(entries, -reach, reach).astype(held_as)


def setup_inputs(seed: int = 0) -> dict:
    streams_of = jax.random.split(jax.random.key(seed), 8)
    return {
        "pressure_field": gaussian(streams_of[0], (NZ, 2 * F), 1.0, 6.0, ((0, 2), (1, 16))),
        "block_main": gaussian(streams_of[1], (NZ, 3, 2, BS), (12 * BS) ** -0.5, 0.15625, ((0, 2),)),
        "block_coupled": gaussian(streams_of[2], (NZ, 3, 2, BS), (12 * BS) ** -0.5, 0.15625, ((0, 2),)),
        "coupling": gaussian(streams_of[3], (2 * F,), 0.5, 3.0, ((0, 16),), jnp.float32),
        "frequencies": jnp.clip(jax.random.uniform(streams_of[4], (F,), jnp.float32, 1.0, 1024.0), 1.0, 1024.0),
        "receivers": touch_ends(jax.random.randint(streams_of[5], (R,), 0, NZ), jax.random.fold_in(streams_of[5], 1), 0, NZ - 1).astype(jnp.int32),
        "floors": touch_ends(jax.random.randint(streams_of[6], (STEPS,), NZ // 4, NZ), jax.random.fold_in(streams_of[6], 1), NZ // 4, NZ - 1).astype(jnp.int32),
    }


def apply_blocks(blocks, padded):
    block_count = blocks.shape[0]
    width = padded.shape[1]
    stacked = padded.reshape(block_count + 2, BS, width)
    neighbours = jnp.stack([stacked[:-2], stacked[1:-1], stacked[2:]], axis=1)
    product = jnp.einsum('bikrj,bkjc->rbic', blocks, neighbours, precision=lax.Precision.HIGHEST)
    real_part = product[0].reshape(block_count * BS, width)
    imag_part = product[1].reshape(block_count * BS, width // 2, 2)
    rotated = jnp.stack([-imag_part[..., 1], imag_part[..., 0]], axis=-1).reshape(block_count * BS, width)
    return real_part + rotated

def couple_terms(values, weights):
    height = values.shape[0]
    paired = values.reshape(height, -1, 2)
    wpair = weights.reshape(-1, 2)
    real_part = wpair[:, 0] * paired[..., 0] - wpair[:, 1] * paired[..., 1]
    imag_part = wpair[:, 0] * paired[..., 1] + wpair[:, 1] * paired[..., 0]
    return jnp.stack([real_part, imag_part], axis=-1).reshape(height, -1)

def make_basis(freq_values, sample_times):
    phase = jnp.mod(freq_values[:, None] * sample_times[None, :], jnp.float32(NT)) / jnp.float32(NT)
    angle = 2.0 * math.pi * phase
    stacked = jnp.stack([jnp.cos(angle), -jnp.sin(angle)], axis=1)
    return stacked.reshape(2 * freq_values.shape[0], sample_times.shape[0]).astype(jnp.bfloat16)

def reference(pressure_field, block_main, block_coupled, coupling, frequencies, receivers, floors):
    block_count = NZ // BS
    main_blocks = block_main.astype(jnp.float32).reshape(block_count, BS, 3, 2, BS)
    side_blocks = block_coupled.astype(jnp.float32).reshape(block_count, BS, 3, 2, BS)
    grouped = pressure_field.reshape(NZ, N_FREQ, 2 * F_DEV).transpose(1, 0, 2)
    pairs = coupling.reshape(N_FREQ, 2 * F_DEV)
    freq_groups = frequencies.reshape(N_FREQ, F_DEV)
    depth_index = jnp.arange(NZ, dtype=jnp.int32)
    sample_times = jnp.arange(NT, dtype=jnp.float32)

    def one_group(running, group_items):
        columns, weights, freq_values = group_items
        for step in range(STEPS):
            padded = jnp.pad(columns.astype(jnp.float32), ((BS, BS), (0, 0)))
            combined = apply_blocks(main_blocks, padded) + couple_terms(apply_blocks(side_blocks, padded), weights)
            damping = jnp.where(depth_index >= floors[step], 0.5, 1.0).astype(jnp.float32)
            columns = (damping[:, None] * combined).astype(jnp.bfloat16)
        picked = jnp.take(columns, receivers, axis=0)
        basis_table = make_basis(freq_values, sample_times)
        return (running + jnp.dot(picked, basis_table, preferred_element_type=jnp.float32), None)
    running, _ = lax.scan(one_group, jnp.zeros((R, NT), jnp.float32), (grouped, pairs, freq_groups))
    return running * (1.0 / math.sqrt(F))
```

```python
import functools
import math

import jax
import jax.numpy as jnp
from jax import lax
from jax.experimental import pallas as pl
from jax.experimental.pallas import tpu as pltpu
from jax.sharding import PartitionSpec as P

NT = 2048
STEPS = 4

COS_TERMS = (1.0, -19.739208221435547, 64.93939208984375, -85.45665740966797,
             60.242130279541016, -26.4046688079834, 7.800131320953369, -1.453112244606018)
SIN_TERMS = (6.2831854820251465, -41.34170150756836, 81.6052474975586, -76.70580291748047,
             42.05775451660156, -15.086565017700195, 3.7813189029693604, -0.6207787394523621)

MESH = pl.DeviceIdType.MESH
F32 = jnp.float32
BF16 = jnp.bfloat16


def poly(terms, z):
    total = jnp.full_like(z, terms[-1])
    for term in terms[-2::-1]:
        total = total * z + F32(term)
    return total


def unroll_of(count, choices=(5, 4, 3, 2, 1)):
    return next(c for c in choices if count % c == 0)


def split_rows(rows, parts):
    unit = 16
    units = rows // unit
    cuts = [round(units * i / parts) * unit for i in range(parts)] + [rows]
    return [(cuts[i], cuts[i + 1] - cuts[i]) for i in range(parts)]


def plan_of(rows, bits):
    parts = min(3, max(1, bits - 1))
    plan = []
    for i, (start, count) in enumerate(split_rows(rows, parts)):
        low = list(range(bits - 1))
        order = low[i:] + low[:i] + [bits - 1]
        plan.append((start, count, order))
    return plan


def kernel(depth_n, freq_n, bits, factor, plan,
           field, main_hbm, side_hbm, weights, freqs, receivers, floors, out,
           raw_main, raw_side, spread, ops, w_buf, final, halo, picked, owned, pick_in,
           basis, sums, *rest):
    n_parts = len(plan)
    send_bufs = rest[:n_parts]
    recv_bufs = rest[n_parts:2 * n_parts]
    load_sem, halo_send, halo_recv, pick_send, pick_recv, rs_send, rs_recv = rest[2 * n_parts:]
    rows, width = field.shape
    half = width // 2
    bs = raw_main.shape[1]
    kc = 6
    nb = rows // bs
    bw = 2 * bs
    me_d = lax.axis_index("depth")
    me_f = lax.axis_index("freq")
    first_row = me_d * rows

    for which, (src, dst) in enumerate(((main_hbm, raw_main), (side_hbm, raw_side))):
        def start(b, carry, src=src, dst=dst, which=which):
            at = pl.ds(pl.multiple_of(b * kc * bs, kc * bs), kc * bs)
            pltpu.make_async_copy(src.at[at], dst.at[at], load_sem.at[which, b]).start()
            return carry
        lax.fori_loop(0, nb, start, 0)

    barrier = pltpu.get_barrier_semaphore()
    for off in range(1, depth_n):
        pl.semaphore_signal(barrier, inc=1, device_id={"depth": lax.rem(me_d + off, depth_n)},
                            device_id_type=MESH)
    partners = []
    for j in range(bits):
        mine = lax.rem(me_f // (1 << j), 2)
        partners.append((mine, me_f + (1 - 2 * mine) * (1 << j)))
        pl.semaphore_signal(barrier, inc=1, device_id={"freq": partners[j][1]}, device_id_type=MESH)

    def put_w(parity, b, re, im):
        base = pl.multiple_of((b + 1) * bw, bw)
        top, low = pl.ds(base, bs), pl.ds(pl.multiple_of(base + bs, bs), bs)
        w_buf[parity, top, :half] = re
        w_buf[parity, top, half:] = im
        w_buf[parity, low, :half] = -im
        w_buf[parity, low, half:] = re

    from_col = lax.broadcasted_iota(jnp.int32, (width, width), 0)
    to_col = lax.broadcasted_iota(jnp.int32, (width, width), 1)
    wanted = jnp.where(to_col < half, 2 * to_col, 2 * (to_col - half) + 1)
    order = jnp.where(from_col == wanted, 1.0, 0.0).astype(BF16)

    def enter(b, carry):
        at = pl.ds(pl.multiple_of(b * bs, bs), bs)
        got = jnp.dot(field[at, :], order, preferred_element_type=F32).astype(BF16)
        put_w(0, b, got[:, :half], got[:, half:])
        return carry

    enter(0, 0)
    enter(nb - 1, 0)
    lax.fori_loop(1, nb - 1, enter, 0, unroll=2)
    zero_edge = jnp.zeros((bw, width), BF16)
    for parity in range(2):
        w_buf[parity, :bw, :] = zero_edge
        w_buf[parity, (nb + 1) * bw:, :] = zero_edge

    pl.semaphore_wait(barrier, depth_n - 1 + bits)

    def halo_copy(step, side):
        edge = (1 if side == 0 else nb) * bw
        to = lax.rem(me_d + (depth_n - 1 if side == 0 else 1), depth_n)
        return pltpu.make_async_remote_copy(
            src_ref=w_buf.at[step % 2, pl.ds(edge, bw)],
            dst_ref=halo.at[step, side],
            send_sem=halo_send.at[step, side],
            recv_sem=halo_recv.at[step, side],
            device_id={"depth": to},
            device_id_type=MESH,
        )

    has_above = me_d > 0
    has_below = me_d < depth_n - 1

    def halo_start(step):
        if depth_n == 1:
            return

        @pl.when(has_above)
        def _():
            halo_copy(step, 0).start()

        @pl.when(has_below)
        def _():
            halo_copy(step, 1).start()

    def halo_finish(step):
        if depth_n == 1:
            return

        @pl.when(has_above)
        def _():
            halo_copy(step, 0).wait_send()
            halo_copy(step, 1).wait_recv()
            w_buf[step % 2, :bw, :] = halo[step, 1]

        @pl.when(has_below)
        def _():
            halo_copy(step, 1).wait_send()
            halo_copy(step, 0).wait_recv()
            w_buf[step % 2, (nb + 1) * bw:, :] = halo[step, 0]

    halo_start(0)

    times = out.shape[1]
    lane = lax.broadcasted_iota(jnp.int32, (half, times), 1)

    def basis_of(c, carry):
        n = (c * times + lane).astype(F32)
        y = (freqs[...] * n) * F32(1.0 / NT)
        p = y - jnp.floor(y)
        r = jnp.where(p > 0.5, p - 1.0, p)
        z = r * r
        basis[c, :half, :] = poly(COS_TERMS, z).astype(BF16)
        basis[c, half:, :] = (-(r * poly(SIN_TERMS, z))).astype(BF16)
        return carry

    lax.fori_loop(0, freq_n, basis_of, 0)

    wr = weights[0:1, :]
    wi = weights[1:2, :]
    row_iota = lax.broadcasted_iota(jnp.int32, (bs, half), 0)

    def multiply(step, b):
        parity = step % 2
        near = pl.ds(pl.multiple_of(b * bw, bw), 3 * bw)
        acc = jnp.dot(ops[b], w_buf[parity, near, :], preferred_element_type=F32)
        m, c = acc[:bs], acc[bs:]
        re = m[:, :half] + wr * c[:, :half] - wi * c[:, half:]
        im = m[:, half:] + wr * c[:, half:] + wi * c[:, :half]
        damp = jnp.where(row_iota + (first_row + b * bs) >= floors[step], F32(0.5), F32(1.0))
        re = (damp * re).astype(BF16)
        im = (damp * im).astype(BF16)
        if step == STEPS - 1:
            at = pl.ds(pl.multiple_of(b * bs, bs), bs)
            final[at, :half] = re
            final[at, half:] = im
        else:
            put_w(1 - parity, b, re, im)

    def prepare(b):
        at = pl.ds(pl.multiple_of(b * kc * bs, kc * bs), kc * bs)
        for which, (src, dst) in enumerate(((main_hbm, raw_main), (side_hbm, raw_side))):
            pltpu.make_async_copy(src.at[at], dst.at[at], load_sem.at[which, b]).wait()
            spread[which] = dst[at, :].astype(F32)
            for piece in range(kc):
                ops[b, which * bs:(which + 1) * bs, piece * bs:(piece + 1) * bs] = spread[
                    which, pl.ds(piece, bs, stride=kc), :].astype(BF16)

    prepare(0)
    prepare(nb - 1)
    prepare(1)

    def first_step(b, carry):
        multiply(0, b)

        @pl.when(b + 1 < nb - 1)
        def _():
            prepare(b + 1)

        return carry

    lax.fori_loop(1, nb - 1, first_step, 0)
    halo_finish(0)
    multiply(0, 0)
    multiply(0, nb - 1)
    for step in range(1, STEPS):
        multiply(step, 1)
        multiply(step, 2)
        halo_start(step)

        def inner(b, carry, step=step):
            multiply(step, b)
            return carry

        lax.fori_loop(3, nb - 1, inner, 0, unroll=unroll_of(nb - 4))
        halo_finish(step)
        multiply(step, 0)
        multiply(step, nb - 1)

    here = out.shape[0]
    chunk = min(rows, 1024)

    def pick(owner):
        at = pl.ds(pl.multiple_of(owner * here, here), here)
        local = receivers[at, :] - first_row
        total = jnp.zeros((here, width), F32)
        for base in range(0, rows, chunk):
            marks = [
                jnp.where(local == lax.broadcasted_iota(jnp.int32, local.shape, 1) + (base + sub),
                          1.0, 0.0).astype(BF16)
                for sub in range(0, chunk, local.shape[1])
            ]
            total = total + jnp.dot(jnp.concatenate(marks, axis=1), final[base:base + chunk, :],
                                    preferred_element_type=F32)
        return total

    def pick_copy(off):
        return pltpu.make_async_remote_copy(
            src_ref=picked.at[off - 1],
            dst_ref=pick_in.at[off - 1],
            send_sem=pick_send.at[off - 1],
            recv_sem=pick_recv.at[off - 1],
            device_id={"depth": lax.rem(me_d + off, depth_n)},
            device_id_type=MESH,
        )

    for off in range(1, depth_n):
        picked[off - 1] = pick(lax.rem(me_d + off, depth_n)).astype(BF16)
    for off in range(1, depth_n):
        pick_copy(off).start()
    mine_rows = pick(me_d)
    for off in range(1, depth_n):
        pick_copy(off).wait()
        mine_rows = mine_rows + pick_in[off - 1].astype(F32)
    owned[...] = mine_rows.astype(BF16)

    def chunk_at(part_order, q):
        c = 0
        for t, j in enumerate(part_order):
            c = c + lax.rem(q // (1 << (bits - 1 - t)), 2) * (1 << j)
        return c

    def partial(part, q):
        start, count, part_order = plan[part]
        return jnp.dot(owned[start:start + count, :], basis[chunk_at(part_order, q)],
                       preferred_element_type=F32)

    def offset_of(stage):
        return freq_n - (freq_n >> stage)

    def rs_copy(part, stage):
        size = freq_n >> (stage + 1)
        at = pl.ds(offset_of(stage), size)
        j = plan[part][2][stage]
        return pltpu.make_async_remote_copy(
            src_ref=send_bufs[part].at[at],
            dst_ref=recv_bufs[part].at[at],
            send_sem=rs_send.at[part, stage],
            recv_sem=rs_recv.at[part, stage],
            device_id={"freq": partners[j][1]},
            device_id_type=MESH,
        )

    if bits == 0:
        out[...] = jnp.dot(owned[...], basis[0], preferred_element_type=F32) * factor
        return

    def sweep(size, body):
        def one(q, carry):
            body(q)
            return carry
        lax.fori_loop(0, size, one, 0, unroll=min(2, size))

    size = freq_n // 2
    for part in range(n_parts):
        mine = partners[plan[part][2][0]][0]

        def fill(q, part=part, mine=mine):
            send_bufs[part][q] = partial(part, (1 - mine) * size + q).astype(BF16)

        sweep(size, fill)
    for part in range(n_parts):
        rs_copy(part, 0).start()
    for part in range(n_parts):
        start, count, _ = plan[part]
        mine = partners[plan[part][2][0]][0]

        def keep(q, part=part, mine=mine, start=start, count=count):
            sums[q, start:start + count, :] = partial(part, mine * size + q)

        sweep(size, keep)
    for stage in range(bits):
        size = freq_n >> (stage + 1)
        base = offset_of(stage)
        last = stage == bits - 1
        for part in range(n_parts):
            start, count, part_order = plan[part]
            rs_copy(part, stage).wait()
            at = slice(start, start + count)
            if last:
                out[at, :] = (sums[0, at, :] + recv_bufs[part][base].astype(F32)) * factor
                continue
            nxt = size // 2
            mine = partners[part_order[stage + 1]][0]
            into = offset_of(stage + 1)

            def send(q, part=part, at=at, mine=mine, nxt=nxt, base=base, into=into):
                k = (1 - mine) * nxt + q
                send_bufs[part][into + q] = (
                    sums[k, at, :] + recv_bufs[part][base + k].astype(F32)).astype(BF16)

            sweep(nxt, send)
            rs_copy(part, stage + 1).start()

            def hold(q, part=part, at=at, mine=mine, nxt=nxt, base=base):
                k = mine * nxt + q
                sums[q, at, :] = sums[k, at, :] + recv_bufs[part][base + k].astype(F32)

            sweep(nxt, hold)


def local(depth_n, freq_n, pressure_field, block_main, block_coupled, coupling, frequencies,
          receivers, floors):
    rows, width = pressure_field.shape
    bs = block_main.shape[3]
    half = width // 2
    nb = rows // bs
    bits = freq_n.bit_length() - 1
    here = receivers.shape[0] // depth_n
    times = NT // freq_n
    factor = 1.0 / math.sqrt(frequencies.shape[0])
    plan = plan_of(here, bits)
    weights = coupling.reshape(half, 2).T
    own = lax.dynamic_slice_in_dim(frequencies, lax.axis_index("freq") * half, half)
    freqs = jnp.broadcast_to(own[:, None], (half, times))
    spots = jnp.broadcast_to(receivers[:, None], (receivers.shape[0], bs))
    vmem = pl.BlockSpec(memory_space=pltpu.VMEM)
    hbm = pl.BlockSpec(memory_space=pl.ANY)
    away = max(depth_n - 1, 1)
    slots = max(freq_n - 1, 1)
    return pl.pallas_call(
        functools.partial(kernel, depth_n, freq_n, bits, factor, plan),
        out_shape=jax.ShapeDtypeStruct((here, times), F32),
        in_specs=[vmem, hbm, hbm, vmem, vmem, vmem, pl.BlockSpec(memory_space=pltpu.SMEM)],
        out_specs=vmem,
        scratch_shapes=[
            pltpu.VMEM((rows * 6, bs), BF16),
            pltpu.VMEM((rows * 6, bs), BF16),
            pltpu.VMEM((2, 6 * bs, bs), F32),
            pltpu.VMEM((nb, 2 * bs, 6 * bs), BF16),
            pltpu.VMEM((2, (nb + 2) * 2 * bs, width), BF16),
            pltpu.VMEM((rows, width), BF16),
            pltpu.VMEM((STEPS, 2, 2 * bs, width), BF16),
            pltpu.VMEM((away, here, width), BF16),
            pltpu.VMEM((here, width), BF16),
            pltpu.VMEM((away, here, width), BF16),
            pltpu.VMEM((freq_n, width, times), BF16),
            pltpu.VMEM((max(freq_n // 2, 1), here, times), F32),
            *[pltpu.VMEM((slots, count, times), BF16) for _, count, _ in plan],
            *[pltpu.VMEM((slots, count, times), BF16) for _, count, _ in plan],
            pltpu.SemaphoreType.DMA((2, nb)),
            pltpu.SemaphoreType.DMA((STEPS, 2)),
            pltpu.SemaphoreType.DMA((STEPS, 2)),
            pltpu.SemaphoreType.DMA((away,)),
            pltpu.SemaphoreType.DMA((away,)),
            pltpu.SemaphoreType.DMA((len(plan), max(bits, 1))),
            pltpu.SemaphoreType.DMA((len(plan), max(bits, 1))),
        ],
        compiler_params=pltpu.CompilerParams(
            collective_id=0, has_side_effects=True, vmem_limit_bytes=64 * 1024 * 1024 - 128 * 1024
        ),
    )(
        pressure_field,
        block_main.reshape(rows * 6, bs),
        block_coupled.reshape(rows * 6, bs),
        weights,
        freqs,
        spots,
        floors,
    )


def solution(mesh):
    in_specs = (
        P("depth", "freq"),
        P("depth", None, None, None),
        P("depth", None, None, None),
        P("freq"),
        P(),
        P(),
        P(),
    )
    body = functools.partial(local, mesh.shape["depth"], mesh.shape["freq"])
    return jax.shard_map(body, mesh=mesh, in_specs=in_specs, out_specs=P("depth", "freq"),
                         check_vma=False)
```
